16 devices in a mesh: ep: 16 (over z, y, x, core).
Axes of the slice: x: 2, y: 2, z: 2, core: 2. Of those that a mesh axis runs over, the one named last changes fastest.
Arguments:
- x_tok: bfloat16 [24576, 1024], P('ep')
- route_idx: int32 [24576, 8], P('ep')
- gates: bfloat16 [24576, 8], P('ep')
- dy_tok: bfloat16 [24576, 1024], P('ep')
- w_gate: bfloat16 [32, 1024, 512], P('ep')
- w_up: bfloat16 [32, 1024, 512], P('ep')
- w_down: bfloat16 [32, 512, 1024], P('ep')
Outputs:
- output 1: bfloat16 [24576, 1024], P('ep')
- output 2: bfloat16 [24576, 1024], P('ep')
- output 3: float32 [32, 1024, 512], P('ep')
- output 4: float32 [32, 1024, 512], P('ep')
- output 5: float32 [32, 512, 1024], P('ep')
All inputs are finite; a program needn't handle non-finite values.
Results may differ from the reference program's by a relative error of at most 0.0104009.
Values are sent between devices in bfloat16 or wider.
A program may use at most 1 GiB of HBM per device.

```python
import jax
import jax.numpy as jnp
from jax import lax

EXPERTS = 32
TOP_K = 8
MODEL_DIM = 1024
EXPERT_FF = 512
TOK_DEV = 1536
EP_SIZE = 16

TOKENS = EP_SIZE * TOK_DEV
SLOT_CAP = 2 * TOK_DEV * TOP_K // (EXPERTS - 2)
HOT_CAP = TOK_DEV // 2
WINDOW = EP_SIZE * max(SLOT_CAP, HOT_CAP)


def source_routes(src_key, count_one, count_two):
    sub_keys = jax.random.split(src_key, 3)
    assigns = TOK_DEV * TOP_K
    remaining = assigns - count_one - count_two
    full_pick = jax.random.randint(sub_keys[0], (), 0, EXPERTS - 2)
    tickets = jax.random.permutation(sub_keys[1], (EXPERTS - 3) * SLOT_CAP)
    others = jnp.sum((tickets < remaining - SLOT_CAP).reshape(EXPERTS - 3, SLOT_CAP), axis=1).astype(jnp.int32)
    places = jnp.arange(EXPERTS - 3) + (jnp.arange(EXPERTS - 3) >= full_pick).astype(jnp.int32)
    middle = jnp.zeros((EXPERTS - 2,), jnp.int32).at[places].set(others).at[full_pick].set(SLOT_CAP)
    counts = jnp.concatenate([count_one[None], middle, count_two[None]]).astype(jnp.int32)
    bounds = jnp.cumsum(counts)
    listing = jnp.searchsorted(bounds, jnp.arange(assigns), side='right').astype(jnp.int32)
    route_table = listing.reshape(TOP_K, TOK_DEV).T
    tok_order = jax.random.permutation(sub_keys[2], TOK_DEV)
    return route_table[tok_order]


def draw_routing(route_key):
    sub_keys = jax.random.split(route_key, 4)
    hot_one = jax.random.randint(sub_keys[0], (EP_SIZE,), HOT_CAP // 4, HOT_CAP + 1)
    hot_two = jax.random.randint(sub_keys[1], (EP_SIZE,), HOT_CAP // 4, HOT_CAP + 1)
    full_src = jax.random.randint(sub_keys[2], (2,), 0, EP_SIZE)
    hot_one = hot_one.at[full_src[0]].set(HOT_CAP)
    hot_two = hot_two.at[full_src[1]].set(HOT_CAP)
    src_keys = jax.random.split(sub_keys[3], EP_SIZE)
    routes = jax.vmap(source_routes)(src_keys, hot_one, hot_two)
    return routes.reshape(TOKENS, TOP_K)


def setup_inputs(seed: int = 0) -> dict:
    root_key = jax.random.key(seed)
    sub_keys = jax.random.split(root_key, 7)
    x_tok = jax.random.normal(sub_keys[0], (TOKENS, MODEL_DIM), jnp.float32)
    route_idx = draw_routing(sub_keys[1])
    gates = jax.random.uniform(sub_keys[2], (TOKENS, TOP_K), jnp.float32, 0.3, 1.0)
    dy_tok = jax.random.normal(sub_keys[3], (TOKENS, MODEL_DIM), jnp.float32)
    w_gate = jax.random.normal(sub_keys[4], (EXPERTS, MODEL_DIM, EXPERT_FF), jnp.float32) * MODEL_DIM ** -0.5
    w_up = jax.random.normal(sub_keys[5], (EXPERTS, MODEL_DIM, EXPERT_FF), jnp.float32) * MODEL_DIM ** -0.5
    w_down = jax.random.normal(sub_keys[6], (EXPERTS, EXPERT_FF, MODEL_DIM), jnp.float32) * EXPERT_FF ** -0.5
    return {'x_tok': x_tok.astype(jnp.bfloat16), 'route_idx': route_idx, 'gates': gates.astype(jnp.bfloat16), 'dy_tok': dy_tok.astype(jnp.bfloat16), 'w_gate': w_gate.astype(jnp.bfloat16), 'w_up': w_up.astype(jnp.bfloat16), 'w_down': w_down.astype(jnp.bfloat16)}


def reference(x_tok, route_idx, gates, dy_tok, w_gate, w_up, w_down):
    flat_route = route_idx.reshape(-1)
    sort_order = jnp.argsort(flat_route, stable=True).astype(jnp.int32)
    counts = jnp.sum((flat_route[:, None] == jnp.arange(EXPERTS)[None, :]).astype(jnp.int32), axis=0)
    starts = jnp.cumsum(counts) - counts
    padded = jnp.concatenate([sort_order, jnp.full((WINDOW,), TOKENS * TOP_K, jnp.int32)])
    flat_gate = gates.reshape(-1)

    def one_expert(acc_pair, expert):
        y_acc, dx_acc = acc_pair
        pick_idx = lax.dynamic_slice(padded, (starts[expert],), (WINDOW,))
        valid_row = jnp.arange(WINDOW) < counts[expert]
        pick_idx = jnp.where(valid_row, pick_idx, TOKENS * TOP_K)
        tok_idx = pick_idx // TOP_K
        gate_rows = jnp.take(flat_gate, pick_idx, mode='fill', fill_value=0).astype(jnp.float32)
        x_rows = jnp.take(x_tok, tok_idx, axis=0, mode='fill', fill_value=0)
        dy_rows = jnp.take(dy_tok, tok_idx, axis=0, mode='fill', fill_value=0)
        gate_mat = w_gate[expert]
        up_mat = w_up[expert]
        down_mat = w_down[expert]
        u_val = jnp.dot(x_rows, gate_mat, preferred_element_type=jnp.float32)
        v_val = jnp.dot(x_rows, up_mat, preferred_element_type=jnp.float32)
        sig_u = jax.nn.sigmoid(u_val)
        act_rows = (u_val * sig_u * v_val).astype(jnp.bfloat16)
        out_rows = jnp.dot(act_rows, down_mat, preferred_element_type=jnp.float32).astype(jnp.bfloat16)
        d_out = (gate_rows[:, None] * dy_rows.astype(jnp.float32)).astype(jnp.bfloat16)
        d_act = jnp.dot(d_out, down_mat.T, preferred_element_type=jnp.float32)
        d_u = (d_act * v_val * sig_u * (1.0 + u_val * (1.0 - sig_u))).astype(jnp.bfloat16)
        d_v = (d_act * u_val * sig_u).astype(jnp.bfloat16)
        dx_rows = (jnp.dot(d_u, gate_mat.T, preferred_element_type=jnp.float32) + jnp.dot(d_v, up_mat.T, preferred_element_type=jnp.float32)).astype(jnp.bfloat16)
        y_acc = y_acc.at[tok_idx].add(gate_rows[:, None] * out_rows.astype(jnp.float32), mode='drop')
        dx_acc = dx_acc.at[tok_idx].add(dx_rows.astype(jnp.float32), mode='drop')
        grads = (jnp.dot(x_rows.T, d_u, preferred_element_type=jnp.float32), jnp.dot(x_rows.T, d_v, preferred_element_type=jnp.float32), jnp.dot(act_rows.T, d_out, preferred_element_type=jnp.float32))
        return (y_acc, dx_acc), grads

    zero_acc = (jnp.zeros((TOKENS, MODEL_DIM), jnp.float32), jnp.zeros((TOKENS, MODEL_DIM), jnp.float32))
    (y_acc, dx_acc), (dw_gate, dw_up, dw_down) = lax.scan(one_expert, zero_acc, jnp.arange(EXPERTS))
    return y_acc.astype(jnp.bfloat16), dx_acc.astype(jnp.bfloat16), dw_gate, dw_up, dw_down
```

```python
import functools

import jax
import jax.numpy as jnp
from jax import lax
from jax.experimental import pallas as pl
from jax.experimental.pallas import tpu as pltpu
from jax.sharding import PartitionSpec as P


BF = jnp.bfloat16
F32 = jnp.float32
TILE = 256
GROUP = 8
EXPERT_ORDER = ((4, 0), (8, 1), (12, 0), (12, 1), (8, 0), (4, 1), (0, 0), (0, 1))


def dot_nt(lhs, rhs):
    return lax.dot_general(lhs, rhs, (((1,), (1,)), ((), ())), preferred_element_type=F32)


def dot_tn(lhs, rhs):
    return lax.dot_general(lhs, rhs, (((0,), (0,)), ((), ())), preferred_element_type=F32)


def dot_nn(lhs, rhs):
    return jnp.dot(lhs, rhs, preferred_element_type=F32)


def gather_kernel(lanes, total, tile_e, tile_l, starts, ends, tok, gate, x_tab, dy_tab, x_out, g_out, x_stage, g_stage):
    step = pl.program_id(0)

    @pl.when(step < total[0])
    def _():
        gather_tile(lanes, step, tile_e, tile_l, starts, ends, tok, gate, x_tab, dy_tab, x_out, g_out, x_stage, g_stage)


def gather_tile(lanes, step, tile_e, tile_l, starts, ends, tok, gate, x_tab, dy_tab, x_out, g_out, x_stage, g_stage):
    expert = tile_e[step]
    base = starts[expert] + tile_l[step] * TILE
    end = ends[expert]

    def body(block, carry):
        row0 = block * GROUP
        for q in range(GROUP):
            row = row0 + q
            pos = base + row
            valid = pos < end
            keep = jnp.where(valid, 1.0, 0.0).astype(F32)
            scale = jnp.where(valid, gate[pos], 0.0).astype(F32)
            t = tok[pos]
            dst = pl.ds(pl.multiple_of(row * lanes, lanes), lanes)
            x_stage[dst, :] = x_tab[t].astype(F32) * keep
            g_stage[dst, :] = dy_tab[t].astype(F32) * scale
        return carry

    lax.fori_loop(0, TILE // GROUP, body, 0)
    for c in range(lanes):
        cols = slice(c * 128, (c + 1) * 128)
        x_out[:, cols] = x_stage[pl.ds(c, TILE, stride=lanes), :].astype(BF)
        g_out[:, cols] = g_stage[pl.ds(c, TILE, stride=lanes), :].astype(BF)


def expert_kernel(ff, dim, which, n_tiles, x_ref, g_ref, w_ref, *rest):
    o_ref, dx_ref, p_ref = rest[-3:]
    step = pl.program_id(0)

    @pl.when(step == 0)
    def _():
        p_ref[...] = jnp.zeros_like(p_ref)

    @pl.when(step < n_tiles[which])
    def _():
        expert_tile(ff, dim, x_ref, g_ref, w_ref, o_ref, dx_ref, p_ref)


def expert_tile(ff, dim, x_ref, g_ref, w_ref, o_ref, dx_ref, p_ref):
    x_rows = x_ref[...]
    g_rows = g_ref[...]
    gate_w = w_ref[0:dim, :]
    up_w = w_ref[dim:2 * dim, :]
    u_val = dot_nn(x_rows, gate_w)
    v_val = dot_nn(x_rows, up_w)
    sig = jax.nn.sigmoid(u_val)
    act = (u_val * sig * v_val).astype(BF)
    halves = dim // ff
    d_act = None
    for h in range(halves):
        down = w_ref[2 * dim + h * ff:2 * dim + (h + 1) * ff, :]
        o_ref[:, h * ff:(h + 1) * ff] = dot_nn(act, down).astype(BF)
        part = dot_nt(g_rows[:, h * ff:(h + 1) * ff], down)
        d_act = part if d_act is None else d_act + part
    d_u = (d_act * v_val * sig * (1.0 + u_val * (1.0 - sig))).astype(BF)
    d_v = (d_act * u_val * sig).astype(BF)
    dx_ref[...] = (dot_nt(d_u, gate_w) + dot_nt(d_v, up_w)).astype(BF)
    p_ref[0:dim, :] += dot_tn(x_rows, d_u)
    p_ref[dim:2 * dim, :] += dot_tn(x_rows, d_v)
    for h in range(halves):
        p_ref[2 * dim + h * ff:2 * dim + (h + 1) * ff, :] += dot_tn(act, g_rows[:, h * ff:(h + 1) * ff])


def combine_kernel(lanes, n_tok, use_gate, total, tile_e, tile_l, starts, ends, tok, gate, rows_ref, out_ref, acc, stage, sem):
    step = pl.program_id(0)

    @pl.when(step == 0)
    def _():
        acc[...] = jnp.zeros_like(acc)

    @pl.when(step < total[0])
    def _():
        combine_tile(lanes, n_tok, use_gate, step, tile_e, tile_l, starts, ends, tok, gate, rows_ref, acc, stage)

    @pl.when(step == pl.num_programs(0) - 1)
    def _():
        copy = pltpu.make_async_copy(acc.at[pl.ds(0, n_tok)], out_ref, sem)
        copy.start()
        copy.wait()


def combine_tile(lanes, n_tok, use_gate, step, tile_e, tile_l, starts, ends, tok, gate, rows_ref, acc, stage):
    expert = tile_e[step]
    base = starts[expert] + tile_l[step] * TILE
    end = ends[expert]
    for c in range(lanes):
        stage[pl.ds(c, TILE, stride=lanes), :] = rows_ref[:, c * 128:(c + 1) * 128].astype(F32)

    def body(block, carry):
        row0 = block * GROUP
        dests, sums = [], []
        for q in range(GROUP):
            row = row0 + q
            pos = base + row
            t = jnp.where(pos < end, tok[pos], n_tok + q)
            value = stage[pl.ds(pl.multiple_of(row * lanes, lanes), lanes), :]
            if use_gate:
                value = value * gate[pos]
            dests.append(t)
            sums.append(acc[t] + value)
        for t, total in zip(dests, sums):
            acc[t] = total
        return carry

    lax.fori_loop(0, TILE // GROUP, body, 0)


def solution(mesh):
    n_dev = mesh.shape['ep']

    def permute(value, mask):
        return lax.ppermute(value, 'ep', [(i, i ^ mask) for i in range(n_dev)])

    def local_step(x_tok, route_idx, gates, dy_tok, w_gate, w_up, w_down):
        tok_loc, top_k = route_idx.shape
        dim, ff = w_gate.shape[1], w_gate.shape[2]
        experts = w_gate.shape[0] * n_dev
        lanes = dim // 128
        n_exp = len(EXPERT_ORDER)
        n_tok = 4 * tok_loc
        slot_cap = max(2 * tok_loc * top_k // (experts - 2), tok_loc // 2)
        max_tiles = -(-4 * slot_cap // TILE)
        cap_rows = max_tiles * TILE
        list_len = -(-(n_exp * 4 * slot_cap + TILE) // 1024) * 1024
        me = lax.axis_index('ep')

        pack_w = jnp.concatenate([w_gate, w_up, w_down[:, :, :ff], w_down[:, :, ff:]], axis=1)
        own_a, own_b = pack_w[0], pack_w[1]
        x_rows = x_tok.reshape(tok_loc, lanes, 128)
        dy_rows = dy_tok.reshape(tok_loc, lanes, 128)
        x_xp = permute(x_rows, 2)
        dy_xp = permute(dy_rows, 2)
        wts = {(0, 0): own_a, (0, 1): own_b}
        wts[(8, 0)] = permute(own_a, 8)
        wts[(4, 1)] = permute(own_b, 4)
        wts[(4, 0)] = permute(own_a, 4)
        wts[(8, 1)] = permute(own_b, 8)
        wts[(12, 0)] = permute(wts[(8, 0)], 4)
        wts[(12, 1)] = permute(wts[(4, 1)], 8)

        def gather_sources(own, own_xp):
            pair = jnp.stack([own, own_xp])
            mate = permute(pair, 1)
            return jnp.concatenate([mate, pair], axis=0)

        route_all = gather_sources(route_idx, permute(route_idx, 2)).reshape(n_tok, top_k)
        gates_all = gather_sources(gates, permute(gates, 2)).reshape(n_tok, top_k)
        place = (route_all // 2) ^ me
        slot = jnp.full_like(route_all, n_exp)
        for j, (mask, which) in enumerate(EXPERT_ORDER):
            slot = jnp.where((place == mask) & (route_all % 2 == which), j, slot)
        key = slot * 8192 + jnp.arange(n_tok, dtype=jnp.int32)[:, None]
        sorted_key, sorted_gate = lax.sort((key.reshape(-1), gates_all.astype(F32).reshape(-1)), num_keys=1)
        tok = jnp.pad(sorted_key[:list_len] & 8191, (0, max(0, list_len - n_tok * top_k)))
        gate = jnp.pad(sorted_gate[:list_len], (0, max(0, list_len - n_tok * top_k)))
        counts = jnp.sum((slot.reshape(-1)[:, None] == jnp.arange(n_exp)[None, :]).astype(jnp.int32), axis=0)
        ends = jnp.cumsum(counts)
        starts = ends - counts
        n_tiles = jnp.maximum(1, (counts + TILE - 1) // TILE)
        tile_ends = jnp.cumsum(n_tiles)
        tile_pos = jnp.arange(n_exp * max_tiles, dtype=jnp.int32)
        tile_e = jnp.minimum(jnp.sum((tile_pos[:, None] >= tile_ends[None, :]).astype(jnp.int32), axis=1), n_exp - 1)
        tile_first = jnp.sum(jnp.where(jnp.arange(n_exp)[None, :] < tile_e[:, None], n_tiles[None, :], 0), axis=1)
        tile_l = jnp.minimum(tile_pos - tile_first, max_tiles - 1)
        last = tile_ends[n_exp - 1] - 1
        tile_e = jnp.where(tile_pos > last, n_exp - 1, tile_e)
        tile_l = jnp.where(tile_pos > last, n_tiles[n_exp - 1] - 1, tile_l)
        scalars = (tile_ends[n_exp - 1:], tile_e, tile_l, starts, ends, tok, gate)
        grid_steps = n_exp * max_tiles

        x_tab = gather_sources(x_rows, x_xp).reshape(n_tok, lanes, 128)
        dy_tab = gather_sources(dy_rows, dy_xp).reshape(n_tok, lanes, 128)
        tab_spec = pl.BlockSpec((n_tok, lanes, 128), lambda i, *s: (0, 0, 0), pipeline_mode=pl.Buffered(1))
        row_spec = pl.BlockSpec((TILE, dim), lambda i, n, te, tl, *s: (te[i] * max_tiles + tl[i], 0))
        row_shape = jax.ShapeDtypeStruct((n_exp * cap_rows, dim), BF)
        x_srt, g_srt = pl.pallas_call(
            functools.partial(gather_kernel, lanes),
            grid_spec=pltpu.PrefetchScalarGridSpec(
                num_scalar_prefetch=7, grid=(grid_steps,), in_specs=[tab_spec, tab_spec], out_specs=[row_spec, row_spec],
                scratch_shapes=[pltpu.VMEM((TILE * lanes, 128), F32), pltpu.VMEM((TILE * lanes, 128), F32)]),
            out_shape=[row_shape, row_shape],
            compiler_params=pltpu.CompilerParams(dimension_semantics=('arbitrary',), vmem_limit_bytes=60 * 1024 * 1024),
            cost_estimate=pl.CostEstimate(flops=40 * 10**9, bytes_accessed=100 * 2**20, transcendentals=0),
            name='gather_rows',
        )(*scalars, x_tab, dy_tab)

        o_srt = dx_srt = None
        grads = {}
        for j, place_key in enumerate(EXPERT_ORDER):
            blk = pl.BlockSpec((TILE, dim), lambda i, n, j=j: (j * max_tiles + jnp.minimum(i, n[j] - 1), 0))
            pack = pl.BlockSpec((3 * dim, ff), lambda i, n: (0, 0))
            keep = pl.BlockSpec(memory_space=pl.ANY)
            carried = () if o_srt is None else (o_srt, dx_srt)
            o_srt, dx_srt, grads[place_key] = pl.pallas_call(
                functools.partial(expert_kernel, ff, dim, j),
                grid_spec=pltpu.PrefetchScalarGridSpec(
                    num_scalar_prefetch=1, grid=(max_tiles,),
                    in_specs=[blk, blk, pack] + [keep] * len(carried), out_specs=[blk, blk, pack]),
                out_shape=[row_shape, row_shape, jax.ShapeDtypeStruct((3 * dim, ff), F32)],
                input_output_aliases={4: 0, 5: 1} if carried else {},
                compiler_params=pltpu.CompilerParams(dimension_semantics=('arbitrary',), vmem_limit_bytes=56 * 1024 * 1024),
                cost_estimate=pl.CostEstimate(flops=15 * 10**9, bytes_accessed=20 * 2**20, transcendentals=0),
                name='expert_step',
            )(n_tiles, x_srt, g_srt, wts[place_key], *carried)

        def combine(rows, use_gate):
            return pl.pallas_call(
                functools.partial(combine_kernel, lanes, n_tok, use_gate),
                grid_spec=pltpu.PrefetchScalarGridSpec(
                    num_scalar_prefetch=7, grid=(grid_steps,), in_specs=[row_spec],
                    out_specs=pl.BlockSpec(memory_space=pl.ANY),
                    scratch_shapes=[pltpu.VMEM((n_tok + GROUP, lanes, 128), F32), pltpu.VMEM((TILE * lanes, 128), F32), pltpu.SemaphoreType.DMA]),
                out_shape=jax.ShapeDtypeStruct((n_tok, lanes, 128), F32),
                compiler_params=pltpu.CompilerParams(dimension_semantics=('arbitrary',), vmem_limit_bytes=56 * 1024 * 1024),
                cost_estimate=pl.CostEstimate(flops=20 * 10**9, bytes_accessed=50 * 2**20, transcendentals=0),
                name='combine_rows',
            )(*scalars, rows)

        def settle_rows(part):
            mine = part[2 * tok_loc:] + permute(part[:2 * tok_loc], 1)
            total = mine[:tok_loc] + permute(mine[tok_loc:], 2)
            return total.astype(BF).reshape(tok_loc, dim)

        y_tok = settle_rows(combine(o_srt, True))
        dx_tok = settle_rows(combine(dx_srt, False))

        g_a = grads[(0, 0)] + permute(grads[(4, 0)], 4)
        g_a = g_a + permute(grads[(8, 0)] + permute(grads[(12, 0)], 4), 8)
        g_b = grads[(0, 1)] + permute(grads[(8, 1)], 8)
        g_b = g_b + permute(grads[(4, 1)] + permute(grads[(12, 1)], 8), 4)
        both = jnp.stack([g_a, g_b])
        d_down = jnp.concatenate([both[:, 2 * dim:2 * dim + ff], both[:, 2 * dim + ff:]], axis=2)
        return y_tok, dx_tok, both[:, :dim], both[:, dim:2 * dim], d_down

    return jax.shard_map(local_step, mesh=mesh, in_specs=(P('ep'),) * 7, out_specs=(P('ep'),) * 5, check_vma=False)
```

```python
import functools

import jax
import jax.numpy as jnp
from jax import lax
from jax.experimental import pallas as pl
from jax.experimental.pallas import tpu as pltpu
from jax.sharding import PartitionSpec as P


BF = jnp.bfloat16
F32 = jnp.float32
I32 = jnp.int32
TILE = 256
GROUP = 8
KEY_STEP = 4096
EXPERTS = ((4, 0), (8, 1), (12, 0), (12, 1), (8, 0), (4, 1), (0, 0), (0, 1))
NEAR_ORDER = ((0, 0), (0, 1), (8, 0), (4, 1), (4, 0), (8, 1))
ANY = pl.BlockSpec(memory_space=pl.ANY)


def dot_nt(lhs, rhs):
    return lax.dot_general(lhs, rhs, (((1,), (1,)), ((), ())), preferred_element_type=F32)


def dot_tn(lhs, rhs):
    return lax.dot_general(lhs, rhs, (((0,), (0,)), ((), ())), preferred_element_type=F32)


def dot_nn(lhs, rhs):
    return jnp.dot(lhs, rhs, preferred_element_type=F32)


def gather_kernel(lanes, n_src, total, tok, gate, mate_ref, own_ref, x_out, g_out, table, x_stage, g_stage, sems):
    step = pl.program_id(0)

    @pl.when(step == 0)
    def _():
        copies = [pltpu.make_async_copy(ref, table.at[pl.ds(i * n_src, n_src)], sems.at[i]) for i, ref in enumerate((mate_ref, own_ref))]
        for copy in copies:
            copy.start()
        table[2 * n_src] = jnp.zeros_like(table[2 * n_src])
        for copy in copies:
            copy.wait()

    @pl.when(step < total[0])
    def _():
        base = step * TILE

        def body(block, carry):
            row0 = block * GROUP
            for q in range(GROUP):
                pos = base + row0 + q
                both = table[tok[pos]]
                dst = pl.ds(pl.multiple_of((row0 + q) * lanes, lanes), lanes)
                x_stage[dst, :] = both[:lanes].astype(F32)
                g_stage[dst, :] = both[lanes:].astype(F32) * gate[pos]
            return carry

        lax.fori_loop(0, TILE // GROUP, body, 0)
        for c in range(lanes):
            cols = slice(c * 128, (c + 1) * 128)
            x_out[:, cols] = x_stage[pl.ds(c, TILE, stride=lanes), :].astype(BF)
            g_out[:, cols] = g_stage[pl.ds(c, TILE, stride=lanes), :].astype(BF)


def expert_kernel(ff, dim, which, has_init, n_carried, first_tile, n_tiles, x_ref, g_ref, w_ref, *rest):
    init_ref = rest[0] if has_init else None
    o_ref, dx_ref, p_ref, sem = rest[n_carried + int(has_init):]
    step = pl.program_id(0)

    @pl.when(step == 0)
    def _():
        if has_init:
            pltpu.make_async_copy(init_ref, p_ref, sem).start()
        else:
            def clear(i, carry):
                p_ref[pl.ds(pl.multiple_of(i * 64, 64), 64), :] = jnp.zeros((64, p_ref.shape[1]), F32)
                return carry

            lax.fori_loop(0, p_ref.shape[0] // 64, clear, 0)

    @pl.when(step < n_tiles[which])
    def _():
        x_rows = x_ref[...]
        g_rows = g_ref[...]
        gate_w = w_ref[0:dim, :]
        up_w = w_ref[dim:2 * dim, :]
        u_val = dot_nn(x_rows, gate_w)
        v_val = dot_nn(x_rows, up_w)
        sig = jax.nn.sigmoid(u_val)
        act = (u_val * sig * v_val).astype(BF)
        halves = dim // ff
        d_act = None
        for h in range(halves):
            down = w_ref[2 * dim + h * ff:2 * dim + (h + 1) * ff, :]
            o_ref[:, h * ff:(h + 1) * ff] = dot_nn(act, down).astype(BF)
            part = dot_nt(g_rows[:, h * ff:(h + 1) * ff], down)
            d_act = part if d_act is None else d_act + part
        d_u = (d_act * v_val * sig * (1.0 + u_val * (1.0 - sig))).astype(BF)
        d_v = (d_act * u_val * sig).astype(BF)
        dx_ref[...] = (dot_nt(d_u, gate_w) + dot_nt(d_v, up_w)).astype(BF)
        if has_init:
            @pl.when(step == 0)
            def _():
                pltpu.make_async_copy(init_ref, p_ref, sem).wait()
        p_ref[0:dim, :] += dot_tn(x_rows, d_u)
        p_ref[dim:2 * dim, :] += dot_tn(x_rows, d_v)
        for h in range(halves):
            p_ref[2 * dim + h * ff:2 * dim + (h + 1) * ff, :] += dot_tn(act, g_rows[:, h * ff:(h + 1) * ff])


def combine_kernel(lanes, n_src, use_gate, total, tok, gate, rows_ref, mate_out, own_out, acc, stage, sems):
    step = pl.program_id(0)

    @pl.when(step == 0)
    def _():
        def clear(i, carry):
            acc[pl.ds(pl.multiple_of(i * 8, 8), 8)] = jnp.zeros((8, lanes, 128), F32)
            return carry

        lax.fori_loop(0, acc.shape[0] // 8, clear, 0)

    @pl.when(step < total[0])
    def _():
        base = step * TILE
        for c in range(lanes):
            stage[pl.ds(c, TILE, stride=lanes), :] = rows_ref[:, c * 128:(c + 1) * 128].astype(F32)

        def body(block, carry):
            row0 = block * GROUP
            dests, sums = [], []
            for q in range(GROUP):
                pos = base + row0 + q
                t = tok[pos]
                value = stage[pl.ds(pl.multiple_of((row0 + q) * lanes, lanes), lanes), :]
                if use_gate:
                    value = value * gate[pos]
                dests.append(t)
                sums.append(acc[t] + value)
            for t, total_row in zip(dests, sums):
                acc[t] = total_row
            return carry

        lax.fori_loop(0, TILE // GROUP, body, 0)

    @pl.when(step == pl.num_programs(0) - 1)
    def _():
        copies = [pltpu.make_async_copy(acc.at[pl.ds(i * n_src, n_src)], ref, sems.at[i]) for i, ref in enumerate((mate_out, own_out))]
        for copy in copies:
            copy.start()
        for copy in copies:
            copy.wait()


def solution(mesh):
    n_dev = mesh.shape['ep']

    def permute(value, mask):
        return lax.ppermute(value, 'ep', [(i, i ^ mask) for i in range(n_dev)])

    def layer(x_tok, route_idx, gates, dy_tok, w_gate, w_up, w_down):
        tok_loc, top_k = route_idx.shape
        dim, ff = w_gate.shape[1], w_gate.shape[2]
        experts = w_gate.shape[0] * n_dev
        lanes = dim // 128
        n_exp = len(EXPERTS)
        slot_cap = max(2 * tok_loc * top_k // (experts - 2), tok_loc // 2)
        max_tiles = -(-2 * slot_cap // TILE)
        n_slots = n_exp * max_tiles
        list_len = n_slots * TILE
        n_half = 2 * tok_loc
        me = lax.axis_index('ep')

        routing = jnp.concatenate([route_idx.T.astype(F32), gates.T.astype(F32)], axis=0)
        rt_mate = permute(routing, 1)
        rt_xp = permute(routing, 2)
        rt_xpm = permute(rt_xp, 1)
        pack_w = jnp.concatenate([w_gate, w_up, w_down[:, :, :ff], w_down[:, :, ff:]], axis=1)
        wts = {(0, 0): pack_w[0], (0, 1): pack_w[1]}
        wts[(8, 0)] = permute(wts[(0, 0)], 8)
        wts[(4, 1)] = permute(wts[(0, 1)], 4)
        wts[(4, 0)] = permute(wts[(0, 0)], 4)
        wts[(8, 1)] = permute(wts[(0, 1)], 8)
        wts[(12, 0)] = permute(wts[(8, 0)], 4)
        wts[(12, 1)] = permute(wts[(4, 1)], 8)
        xd_own = jnp.concatenate([x_tok.reshape(tok_loc, lanes, 128), dy_tok.reshape(tok_loc, lanes, 128)], axis=1)
        xd_xp = permute(xd_own, 2)
        xd_mate = permute(xd_own, 1)
        xd_xpm = permute(xd_xp, 1)

        def plan(rt_pair):
            route = jnp.stack([r[:top_k] for r in rt_pair], axis=1).astype(I32)
            gate = jnp.stack([r[top_k:] for r in rt_pair], axis=1)
            place = (route // 2) ^ me
            slot = jnp.full_like(route, n_exp)
            for j, (mask, which) in enumerate(EXPERTS):
                slot = jnp.where((place == mask) & (route % 2 == which), j, slot)
            token = lax.broadcasted_iota(I32, route.shape, 1) * tok_loc + lax.broadcasted_iota(I32, route.shape, 2)
            key = slot * KEY_STEP + token
            counts = jnp.stack([jnp.sum((slot == j).astype(I32)) for j in range(n_exp)])
            n_tiles = jnp.maximum(1, (counts + TILE - 1) // TILE)
            need = n_tiles * TILE - counts
            pad_key = jnp.where(jnp.arange(TILE)[None, :] < need[:, None], jnp.arange(n_exp)[:, None] * KEY_STEP + n_half, n_exp * KEY_STEP)
            keys = jnp.concatenate([key.reshape(-1), pad_key.reshape(-1)])
            vals = jnp.concatenate([gate.reshape(-1), jnp.zeros((n_exp * TILE,), F32)])
            keys, vals = lax.sort((keys, vals), num_keys=1)
            tile_ends = jnp.cumsum(n_tiles)
            return (tile_ends[n_exp - 1:], keys[:list_len] & (KEY_STEP - 1), vals[:list_len]), (tile_ends - n_tiles, n_tiles)

        row_shape = jax.ShapeDtypeStruct((list_len, dim), BF)
        tile_spec = pl.BlockSpec((TILE, dim), lambda i, n, *s: (jnp.minimum(i, n[0] - 1), 0))

        def gather(lists, mate, own):
            return pl.pallas_call(
                functools.partial(gather_kernel, lanes, tok_loc),
                grid_spec=pltpu.PrefetchScalarGridSpec(
                    num_scalar_prefetch=3, grid=(n_slots,), in_specs=[ANY, ANY], out_specs=[tile_spec, tile_spec],
                    scratch_shapes=[pltpu.VMEM((n_half + 8, 2 * lanes, 128), BF), pltpu.VMEM((TILE * lanes, 128), F32), pltpu.VMEM((TILE * lanes, 128), F32), pltpu.SemaphoreType.DMA((2,))]),
                out_shape=[row_shape, row_shape],
                compiler_params=pltpu.CompilerParams(dimension_semantics=('arbitrary',), vmem_limit_bytes=48 * 1024 * 1024),
                name='gather_rows',
            )(*lists, mate, own)

        def expert(key, tiles, rows, carried, init):
            j = EXPERTS.index(key)
            blk = pl.BlockSpec((TILE, dim), lambda i, first, n: (first[j] + jnp.minimum(i, n[j] - 1), 0))
            pack = pl.BlockSpec((3 * dim, ff), lambda i, first, n: (0, 0))
            extra = ([] if init is None else [init]) + list(carried)
            first_alias = 5 + (init is not None)
            return pl.pallas_call(
                functools.partial(expert_kernel, ff, dim, j, init is not None, len(carried)),
                grid_spec=pltpu.PrefetchScalarGridSpec(
                    num_scalar_prefetch=2, grid=(max_tiles,), in_specs=[blk, blk, pack] + [ANY] * len(extra), out_specs=[blk, blk, pack],
                    scratch_shapes=[pltpu.SemaphoreType.DMA]),
                out_shape=[row_shape, row_shape, jax.ShapeDtypeStruct((3 * dim, ff), F32)],
                input_output_aliases={first_alias: 0, first_alias + 1: 1} if carried else {},
                compiler_params=pltpu.CompilerParams(dimension_semantics=('arbitrary',), vmem_limit_bytes=48 * 1024 * 1024),
                name='expert_step',
            )(*tiles, *rows, wts[key], *extra)

        def combine(lists, rows, use_gate):
            block = jax.ShapeDtypeStruct((tok_loc, lanes, 128), F32)
            return pl.pallas_call(
                functools.partial(combine_kernel, lanes, tok_loc, use_gate),
                grid_spec=pltpu.PrefetchScalarGridSpec(
                    num_scalar_prefetch=3, grid=(n_slots,), in_specs=[tile_spec], out_specs=[ANY, ANY],
                    scratch_shapes=[pltpu.VMEM((n_half + 8, lanes, 128), F32), pltpu.VMEM((TILE * lanes, 128), F32), pltpu.SemaphoreType.DMA((2,))]),
                out_shape=[block, block],
                compiler_params=pltpu.CompilerParams(dimension_semantics=('arbitrary',), vmem_limit_bytes=48 * 1024 * 1024),
                name='combine_rows',
            )(*lists, rows)

        lists0, tiles0 = plan((rt_mate, routing))
        lists1, tiles1 = plan((rt_xpm, rt_xp))
        rows0 = gather(lists0, xd_mate, xd_own)
        out0, out1, part, grads = (), (), {}, {}
        for key in NEAR_ORDER:
            *out0, part[key] = expert(key, tiles0, rows0, out0, None)
        rows1 = gather(lists1, xd_xpm, xd_xp)
        for key in EXPERTS:
            if key not in part:
                *out0, part[key] = expert(key, tiles0, rows0, out0, None)
            *out1, grads[key] = expert(key, tiles1, rows1, out1, part[key])

        def settle_rows(which, use_gate):
            mate1, own1 = combine(lists1, out1[which], use_gate)
            to_x = own1 + permute(mate1, 1)
            mate0, own0 = combine(lists0, out0[which], use_gate)
            total = own0 + permute(mate0, 1) + permute(to_x, 2)
            return total.astype(BF).reshape(tok_loc, dim)

        y_tok = settle_rows(0, True)
        dx_tok = settle_rows(1, False)

        g_a = grads[(0, 0)] + permute(grads[(4, 0)], 4)
        g_a = g_a + permute(grads[(8, 0)] + permute(grads[(12, 0)], 4), 8)
        g_b = grads[(0, 1)] + permute(grads[(8, 1)], 8)
        g_b = g_b + permute(grads[(4, 1)] + permute(grads[(12, 1)], 8), 4)
        both = jnp.stack([g_a, g_b])
        d_down = jnp.concatenate([both[:, 2 * dim:2 * dim + ff], both[:, 2 * dim + ff:]], axis=2)
        return y_tok, dx_tok, both[:, :dim], both[:, dim:2 * dim], d_down

    return jax.shard_map(layer, mesh=mesh, in_specs=(P('ep'),) * 7, out_specs=(P('ep'),) * 5, check_vma=False)
```

```python
import functools

import jax
import jax.numpy as jnp
from jax import lax
from jax.experimental import pallas as pl
from jax.experimental.pallas import tpu as pltpu
from jax.sharding import PartitionSpec as P


BF = jnp.bfloat16
F32 = jnp.float32
I32 = jnp.int32
TILE = 256
GROUP = 16
DEPTH = 4
KEY_STEP = 4096
LIST_PART = 1024
EXPERTS = ((4, 0), (8, 1), (0, 0), (0, 1), (8, 0), (4, 1), (12, 0), (12, 1))
CALLS = ((0, 0, 4), (1, 0, 2), (1, 2, 8), (0, 6, 7), (0, 7, 8), (0, 4, 6))
ANY = pl.BlockSpec(memory_space=pl.ANY)


def dot_nt(lhs, rhs):
    return lax.dot_general(lhs, rhs, (((1,), (1,)), ((), ())), preferred_element_type=F32)


def dot_tn(lhs, rhs):
    return lax.dot_general(lhs, rhs, (((0,), (0,)), ((), ())), preferred_element_type=F32)


def dot_nn(lhs, rhs):
    return jnp.dot(lhs, rhs, preferred_element_type=F32)


def tile_rows(t):
    return pl.ds(pl.multiple_of(t * TILE, TILE), TILE)


def list_stream(count, tok_hbm, gate_hbm, tok, gate, sems):
    def copies(c):
        part = pl.ds(pl.multiple_of(c * LIST_PART, LIST_PART), LIST_PART)
        return (pltpu.make_async_copy(tok_hbm.at[part], tok.at[part], sems.at[0, c]),
                pltpu.make_async_copy(gate_hbm.at[part], gate.at[part], sems.at[1, c]))

    def start(c, carry):
        for copy in copies(c):
            copy.start()
        return carry

    def wait(t):
        @pl.when(lax.rem(t, LIST_PART // TILE) == 0)
        def _():
            for copy in copies(lax.div(t, LIST_PART // TILE)):
                copy.wait()

    lax.fori_loop(0, lax.div(count * TILE + LIST_PART - 1, LIST_PART), start, 0)
    return wait


def gather_kernel(lanes, n_src, total, tok_hbm, gate_hbm, piece0, piece1, piece2, piece3, x_out, g_out, table, x_stage, g_stage, x_buf, g_buf, tok, gate, sems, out_sems, list_sems):
    count = total[0]
    half = lanes // 2
    list_wait = list_stream(count, tok_hbm, gate_hbm, tok, gate, list_sems)
    pieces = (piece0, piece1, piece2, piece3)
    copies = [pltpu.make_async_copy(ref, table.at[pl.ds(i * n_src // 2, n_src // 2)], sems.at[i]) for i, ref in enumerate(pieces)]
    for copy in copies:
        copy.start()
    table[2 * n_src] = jnp.zeros_like(table[2 * n_src])
    for copy in copies:
        copy.wait()

    def stores(t, slot):
        return (pltpu.make_async_copy(x_buf.at[slot], x_out.at[tile_rows(t)], out_sems.at[0, slot]),
                pltpu.make_async_copy(g_buf.at[slot], g_out.at[tile_rows(t)], out_sems.at[1, slot]))

    def tile(t, carry):
        slot = lax.rem(t, 2)
        base = t * TILE
        list_wait(t)

        @pl.when(t >= 2)
        def _():
            for copy in stores(t - 2, slot):
                copy.wait()

        def body(block, inner):
            row0 = block * GROUP
            for q in range(0, GROUP, 2):
                pos = base + row0 + q
                pair = [table[tok[pos + i]] for i in range(2)]
                x_pair = [both[:lanes].astype(F32) for both in pair]
                g_pair = [both[lanes:].astype(F32) * gate[pos + i] for i, both in enumerate(pair)]
                for stage, rows in ((x_stage, x_pair), (g_stage, g_pair)):
                    for h in range(2):
                        dst = pl.ds(pl.multiple_of((row0 + q) * half, lanes), lanes)
                        stage[h, dst, :] = jnp.concatenate([row[h * half:(h + 1) * half] for row in rows], axis=0)
            return inner

        lax.fori_loop(0, TILE // GROUP, body, 0)
        for c in range(lanes):
            cols = slice(c * 128, (c + 1) * 128)
            src = (c // half, pl.ds(c % half, TILE, stride=half))
            x_buf[slot, :, cols] = x_stage[src].astype(BF)
            g_buf[slot, :, cols] = g_stage[src].astype(BF)
        for copy in stores(t, slot):
            copy.start()
        return carry

    lax.fori_loop(0, count, tile, 0)
    for back in (2, 1):
        @pl.when(count >= back)
        def _():
            for copy in stores(count - back, lax.rem(count - back, 2)):
                copy.wait()


def pack_kernel(ff, gate_ref, up_ref, down_ref, a_out, b_out, buf, in_sems, out_sems):
    dim = gate_ref.shape[1]
    loads, stores = [], []
    for e, out in enumerate((a_out, b_out)):
        parts = [(gate_ref.at[e], 0, dim), (up_ref.at[e], dim, dim)]
        parts += [(down_ref.at[e, :, pl.ds(h * ff, ff)], 2 * dim + h * ff, ff) for h in range(dim // ff)]
        for i, (src, row, size) in enumerate(parts):
            rows = pl.ds(row, size)
            loads.append(pltpu.make_async_copy(src, buf.at[e, rows], in_sems.at[e, i]))
            stores.append(pltpu.make_async_copy(buf.at[e, rows], out.at[rows], out_sems.at[e, i]))
    for copy in loads:
        copy.start()
    for load, store in zip(loads, stores):
        load.wait()
        store.start()
    for copy in stores:
        copy.wait()


def expert_kernel(ff, dim, j0, n, inits, n_carried, first_tile, n_tiles, x_hbm, g_hbm, *rest):
    w_refs = rest[:n]
    given = list(rest[n:n + 3 * sum(inits)])
    init_refs = [[given.pop(0) for _ in range(3)] if has else None for has in inits]
    o_hbm, dx_hbm, *rest = rest[n + 3 * sum(inits) + n_carried:]
    p_refs = [rest[3 * i:3 * i + 3] for i in range(n)]
    w_buf, p_buf, x_buf, g_buf, o_buf, dx_buf, w_sem, i_sem, p_sem, in_sem, out_sem = rest[3 * n:]
    base = first_tile[j0]
    count = first_tile[j0 + n - 1] + n_tiles[j0 + n - 1] - base

    def loads(t, slot):
        rows = tile_rows(base + t)
        return (pltpu.make_async_copy(x_hbm.at[rows], x_buf.at[slot], in_sem.at[0, slot]),
                pltpu.make_async_copy(g_hbm.at[rows], g_buf.at[slot], in_sem.at[1, slot]))

    def stores(t, slot):
        rows = tile_rows(base + t)
        return (pltpu.make_async_copy(o_buf.at[slot], o_hbm.at[rows], out_sem.at[0, slot]),
                pltpu.make_async_copy(dx_buf.at[slot], dx_hbm.at[rows], out_sem.at[1, slot]))

    def w_copy(i):
        return pltpu.make_async_copy(w_refs[i], w_buf.at[i % 2], w_sem.at[i % 2])

    def init_copy(i):
        return [pltpu.make_async_copy(init_refs[i][c], p_buf.at[i % 3, pl.ds(c * dim, dim)], i_sem.at[i % 3, c]) for c in range(3)]

    def flush(i):
        return [pltpu.make_async_copy(p_buf.at[i % 3, pl.ds(c * dim, dim)], p_refs[i][c], p_sem.at[i % 3, c]) for c in range(3)]

    def start_all(copies):
        for copy in copies:
            copy.start()

    def wait_all(copies):
        for copy in copies:
            copy.wait()

    for copy in loads(0, 0):
        copy.start()
    for i in range(min(n, 2)):
        w_copy(i).start()
    for i in range(min(n, 2)):
        if inits[i]:
            start_all(init_copy(i))

    def tile(t, carry):
        slot = lax.rem(t, 2)
        place = base + t
        which = jnp.int32(0)
        for i in range(1, n):
            which = which + (place >= first_tile[j0 + i]).astype(I32)

        @pl.when(t + 1 < count)
        def _():
            for copy in loads(t + 1, 1 - slot):
                copy.start()

        for i in range(n):
            @pl.when(place == first_tile[j0 + i])
            def _():
                w_copy(i).wait()
                if 1 <= i < n - 1:
                    w_copy(i + 1).start()
                if i >= 2:
                    wait_all(flush(i - 2))
                if 1 <= i < n - 1 and inits[i + 1]:
                    start_all(init_copy(i + 1))
                if not inits[i]:
                    def clear(r, inner):
                        p_buf[i % 3, pl.ds(pl.multiple_of(r * 64, 64), 64), :] = jnp.zeros((64, ff), F32)
                        return inner

                    lax.fori_loop(0, 3 * dim // 64, clear, 0)

        @pl.when(t >= 2)
        def _():
            for copy in stores(t - 2, slot):
                copy.wait()

        for copy in loads(t, slot):
            copy.wait()
        w_ref = w_buf.at[lax.rem(which, 2)]
        p_ref = p_buf.at[lax.rem(which, 3)]
        x_rows = x_buf[slot]
        g_rows = g_buf[slot]
        gate_w = w_ref[0:dim, :]
        up_w = w_ref[dim:2 * dim, :]
        u_val = dot_nn(x_rows, gate_w)
        v_val = dot_nn(x_rows, up_w)
        sig = jax.nn.sigmoid(u_val)
        act = (u_val * sig * v_val).astype(BF)
        halves = dim // ff
        d_act = None
        for h in range(halves):
            down = w_ref[2 * dim + h * ff:2 * dim + (h + 1) * ff, :]
            o_buf[slot, :, h * ff:(h + 1) * ff] = dot_nn(act, down).astype(BF)
            part = dot_nt(g_rows[:, h * ff:(h + 1) * ff], down)
            d_act = part if d_act is None else d_act + part
        d_u = (d_act * v_val * sig * (1.0 + u_val * (1.0 - sig))).astype(BF)
        d_v = (d_act * u_val * sig).astype(BF)
        dx_buf[slot] = (dot_nt(d_u, gate_w) + dot_nt(d_v, up_w)).astype(BF)
        for copy in stores(t, slot):
            copy.start()
        for i in range(n):
            if inits[i]:
                @pl.when(place == first_tile[j0 + i])
                def _():
                    wait_all(init_copy(i))
        p_ref[0:dim, :] += dot_tn(x_rows, d_u)
        p_ref[dim:2 * dim, :] += dot_tn(x_rows, d_v)
        for h in range(halves):
            p_ref[2 * dim + h * ff:2 * dim + (h + 1) * ff, :] += dot_tn(act, g_rows[:, h * ff:(h + 1) * ff])

        for i in range(n):
            @pl.when(place == first_tile[j0 + i] + n_tiles[j0 + i] - 1)
            def _():
                start_all(flush(i))
        return carry

    lax.fori_loop(0, count, tile, 0)
    for back in (2, 1):
        @pl.when(count >= back)
        def _():
            for copy in stores(count - back, lax.rem(count - back, 2)):
                copy.wait()
    for i in range(max(0, n - 2), n):
        wait_all(flush(i))


def combine_kernel(lanes, n_src, use_gate, total, tok_hbm, gate_hbm, rows_hbm, mate_out, own_out, acc, stage, buf, tok, gate, sems, in_sem, list_sems):
    count = total[0]
    list_wait = list_stream(count, tok_hbm, gate_hbm, tok, gate, list_sems)

    def load(t, slot):
        return pltpu.make_async_copy(rows_hbm.at[tile_rows(t)], buf.at[slot], in_sem.at[slot])

    for ahead in range(DEPTH - 1):
        @pl.when(ahead < count)
        def _():
            load(ahead, ahead).start()

    def clear(i, carry):
        acc[pl.ds(i * 32, 32)] = jnp.zeros((32, lanes, 128), F32)
        return carry

    lax.fori_loop(0, acc.shape[0] // 32, clear, 0)

    def tile(t, carry):
        slot = lax.rem(t, DEPTH)
        base = t * TILE

        @pl.when(t + DEPTH - 1 < count)
        def _():
            load(t + DEPTH - 1, lax.rem(t + DEPTH - 1, DEPTH)).start()

        list_wait(t)
        load(t, slot).wait()
        for c in range(lanes):
            stage[pl.ds(c, TILE, stride=lanes), :] = buf[slot, :, c * 128:(c + 1) * 128].astype(F32)

        def body(block, inner):
            row0 = block * GROUP
            dests, sums = [], []
            for q in range(GROUP):
                pos = base + row0 + q
                t_row = tok[pos]
                value = stage[pl.ds(pl.multiple_of((row0 + q) * lanes, lanes), lanes), :]
                if use_gate:
                    value = value * gate[pos]
                dests.append(t_row)
                sums.append(acc[t_row] + value)
            for t_row, total_row in zip(dests, sums):
                acc[t_row] = total_row
            return inner

        lax.fori_loop(0, TILE // GROUP, body, 0)
        return carry

    lax.fori_loop(0, count, tile, 0)
    copies = [pltpu.make_async_copy(acc.at[pl.ds(i * n_src, n_src)], ref, sems.at[i]) for i, ref in enumerate((mate_out, own_out))]
    for copy in copies:
        copy.start()
    for copy in copies:
        copy.wait()


def finish_kernel(lanes, own_ref, mate_ref, x_ref, out_ref, stage):
    rows = own_ref.shape[0]
    stage[...] = (own_ref[...] + mate_ref[...] + x_ref[...]).reshape(rows * lanes, 128)
    for c in range(lanes):
        out_ref[:, c * 128:(c + 1) * 128] = stage[pl.ds(c, rows, stride=lanes), :].astype(BF)


def solution(mesh):
    n_dev = mesh.shape['ep']

    def permute(value, mask):
        return lax.ppermute(value, 'ep', [(i, i ^ mask) for i in range(n_dev)])

    def layer(x_tok, route_idx, gates, dy_tok, w_gate, w_up, w_down):
        tok_loc, top_k = route_idx.shape
        dim, ff = w_gate.shape[1], w_gate.shape[2]
        experts = w_gate.shape[0] * n_dev
        lanes = dim // 128
        n_exp = len(EXPERTS)
        slot_cap = max(2 * tok_loc * top_k // (experts - 2), tok_loc // 2)
        max_tiles = -(-2 * slot_cap // TILE)
        n_slots = n_exp * max_tiles
        list_len = n_slots * TILE
        n_half = 2 * tok_loc
        me = lax.axis_index('ep')

        routing = jnp.concatenate([route_idx.T.astype(F32), gates.T.astype(F32)], axis=0)
        rt_mate = permute(routing, 1)
        rt_xp = permute(routing, 2)
        rt_xpm = permute(rt_xp, 1)
        w_shape = jax.ShapeDtypeStruct((3 * dim, ff), BF)
        own_a, own_b = pl.pallas_call(
            functools.partial(pack_kernel, ff),
            in_specs=[ANY] * 3, out_specs=[ANY] * 2, out_shape=[w_shape, w_shape],
            scratch_shapes=[pltpu.VMEM((2, 3 * dim, ff), BF), pltpu.SemaphoreType.DMA((2, 4)), pltpu.SemaphoreType.DMA((2, 4))],
            compiler_params=pltpu.CompilerParams(vmem_limit_bytes=16 * 1024 * 1024),
            name='pack_weights',
        )(w_gate, w_up, w_down)
        wts = {(0, 0): own_a, (0, 1): own_b}
        wts[(8, 0)] = permute(wts[(0, 0)], 8)
        wts[(4, 1)] = permute(wts[(0, 1)], 4)
        wts[(4, 0)] = permute(wts[(0, 0)], 4)
        wts[(8, 1)] = permute(wts[(0, 1)], 8)
        wts[(12, 0)] = permute(wts[(8, 0)], 4)
        wts[(12, 1)] = permute(wts[(4, 1)], 8)
        cut = tok_loc // 2
        xd_own, xd_xp, xd_mate, xd_xpm = [], [], [], []
        for i in range(2):
            part = slice(i * cut, (i + 1) * cut)
            xd_own.append(jnp.concatenate([x_tok[part].reshape(cut, lanes, 128), dy_tok[part].reshape(cut, lanes, 128)], axis=1))
            xd_xp.append(permute(xd_own[i], 2))
            xd_mate.append(permute(xd_own[i], 1))
            xd_xpm.append(permute(xd_xp[i], 1))

        rt_all = jnp.stack([jnp.stack([rt_mate, routing]), jnp.stack([rt_xpm, rt_xp])])
        route = rt_all[:, :, :top_k].astype(I32)
        gate_in = rt_all[:, :, top_k:]
        place = (route // 2) ^ me
        slot = jnp.full_like(route, n_exp)
        for j, (mask, which) in enumerate(EXPERTS):
            slot = jnp.where((place == mask) & (route % 2 == which), j, slot)
        token = lax.broadcasted_iota(I32, route.shape, 1) * tok_loc + lax.broadcasted_iota(I32, route.shape, 3)
        first_key = jnp.arange(2, dtype=I32) * (16 * KEY_STEP)
        key = (slot * KEY_STEP + token + first_key[:, None, None, None]).reshape(2, -1)
        counts = jnp.sum((slot.reshape(1, 2, -1) == jnp.arange(n_exp).reshape(n_exp, 1, 1)).astype(I32), axis=2).T
        n_tiles = jnp.maximum(1, (counts + TILE - 1) // TILE)
        need = n_tiles * TILE - counts
        pad_key = jnp.where(jnp.arange(TILE) < need[:, :, None], jnp.arange(n_exp)[:, None] * KEY_STEP + n_half, n_exp * KEY_STEP) + first_key[:, None, None]
        keys = jnp.concatenate([key, pad_key.reshape(2, -1)], axis=1)
        vals = jnp.concatenate([gate_in.reshape(2, -1), jnp.zeros((2, n_exp * TILE), F32)], axis=1)
        keys, vals = lax.sort((keys.reshape(-1), vals.reshape(-1)), num_keys=1)
        per_half = n_half * top_k + n_exp * TILE
        tile_ends = jnp.cumsum(n_tiles, axis=1)
        lists = [(tile_ends[h, n_exp - 1:], keys[h * per_half:][:list_len] & (KEY_STEP - 1), vals[h * per_half:][:list_len]) for h in range(2)]
        tiles = [(tile_ends[h] - n_tiles[h], n_tiles[h]) for h in range(2)]

        row_shape = jax.ShapeDtypeStruct((list_len, dim), BF)
        tile_buf = pltpu.VMEM((2, TILE, dim), BF)
        stage_buf = pltpu.VMEM((TILE * lanes, 128), F32)
        half_buf = pltpu.VMEM((2, TILE * lanes // 2, 128), F32)
        list_bufs = (pltpu.SMEM((list_len,), I32), pltpu.SMEM((list_len,), F32))
        list_sems = pltpu.SemaphoreType.DMA((2, list_len // LIST_PART))

        def gather(lists, pieces):
            return pl.pallas_call(
                functools.partial(gather_kernel, lanes, tok_loc),
                grid_spec=pltpu.PrefetchScalarGridSpec(
                    num_scalar_prefetch=1, grid=(), in_specs=[ANY] * 6, out_specs=[ANY, ANY],
                    scratch_shapes=[pltpu.VMEM((n_half + 8, 2 * lanes, 128), BF), half_buf, half_buf, tile_buf, tile_buf, *list_bufs, pltpu.SemaphoreType.DMA((4,)), pltpu.SemaphoreType.DMA((2, 2)), list_sems]),
                out_shape=[row_shape, row_shape],
                compiler_params=pltpu.CompilerParams(vmem_limit_bytes=48 * 1024 * 1024),
                name='gather_rows',
            )(*lists, *pieces)

        def experts_call(call, tiles, rows, carried, inits):
            _, lo, hi = call
            n = hi - lo
            keys = EXPERTS[lo:hi]
            given = [part for k in keys if k in inits for part in inits[k]]
            extra = [wts[k] for k in keys] + given + list(carried)
            first_alias = 4 + n + len(given)
            grad = jax.ShapeDtypeStruct((dim, ff), F32)
            o_rows, dx_rows, *parts = pl.pallas_call(
                functools.partial(expert_kernel, ff, dim, lo, n, tuple(k in inits for k in keys), len(carried)),
                grid_spec=pltpu.PrefetchScalarGridSpec(
                    num_scalar_prefetch=2, grid=(), in_specs=[ANY] * (2 + len(extra)), out_specs=[ANY] * (2 + 3 * n),
                    scratch_shapes=[pltpu.VMEM((2, 3 * dim, ff), BF), pltpu.VMEM((3, 3 * dim, ff), F32), tile_buf, tile_buf, tile_buf, tile_buf,
                                    pltpu.SemaphoreType.DMA((2,)), pltpu.SemaphoreType.DMA((3, 3)), pltpu.SemaphoreType.DMA((3, 3)), pltpu.SemaphoreType.DMA((2, 2)), pltpu.SemaphoreType.DMA((2, 2))]),
                out_shape=[row_shape, row_shape] + [grad] * (3 * n),
                input_output_aliases={first_alias: 0, first_alias + 1: 1} if carried else {},
                compiler_params=pltpu.CompilerParams(vmem_limit_bytes=56 * 1024 * 1024),
                name='expert_steps',
            )(*tiles, *rows, *extra)
            return (o_rows, dx_rows), {k: tuple(parts[3 * i:3 * i + 3]) for i, k in enumerate(keys)}

        def combine(lists, rows, use_gate):
            block = jax.ShapeDtypeStruct((tok_loc, lanes, 128), F32)
            return pl.pallas_call(
                functools.partial(combine_kernel, lanes, tok_loc, use_gate),
                grid_spec=pltpu.PrefetchScalarGridSpec(
                    num_scalar_prefetch=1, grid=(), in_specs=[ANY] * 3, out_specs=[ANY, ANY],
                    scratch_shapes=[pltpu.VMEM((n_half + 32, lanes, 128), F32), stage_buf, pltpu.VMEM((DEPTH, TILE, dim), BF), *list_bufs, pltpu.SemaphoreType.DMA((2,)), pltpu.SemaphoreType.DMA((DEPTH,)), list_sems]),
                out_shape=[block, block],
                compiler_params=pltpu.CompilerParams(vmem_limit_bytes=48 * 1024 * 1024),
                name='combine_rows',
            )(*lists, rows)

        rows = (gather(lists[0], xd_mate + xd_own), gather(lists[1], xd_xpm + xd_xp))
        outs, grads = [(), ()], {}
        for call in CALLS:
            half = call[0]
            outs[half], parts = experts_call(call, tiles[half], rows[half], outs[half], grads)
            grads = {**grads, **parts}
        out0, out1 = outs
        lists0, lists1 = lists

        def settle_rows(which, use_gate):
            mate1, own1 = combine(lists1, out1[which], use_gate)
            mate1 = permute(mate1, 1)
            to_x = own1 + mate1
            from_x = permute(to_x, 2)
            mate0, own0 = combine(lists0, out0[which], use_gate)
            mate0 = permute(mate0, 1)
            rows_in = pl.BlockSpec((TILE, lanes, 128), lambda i: (i, 0, 0))
            return pl.pallas_call(
                functools.partial(finish_kernel, lanes), grid=(tok_loc // TILE,), in_specs=[rows_in] * 3,
                out_specs=pl.BlockSpec((TILE, dim), lambda i: (i, 0)), out_shape=jax.ShapeDtypeStruct((tok_loc, dim), BF),
                scratch_shapes=[stage_buf], compiler_params=pltpu.CompilerParams(vmem_limit_bytes=24 * 1024 * 1024), name='finish_rows',
            )(own0, mate0, from_x)

        y_tok = settle_rows(0, True)
        dx_tok = settle_rows(1, False)

        totals = []
        for c in range(3):
            def back(key, mask, value=None):
                return permute(grads[key][c] if value is None else value, mask)

            via_a = grads[(8, 0)][c] + back((12, 0), 4)
            via_b = grads[(4, 1)][c] + back((12, 1), 8)
            g_a = grads[(0, 0)][c] + back((4, 0), 4) + back((8, 0), 8, via_a)
            g_b = grads[(0, 1)][c] + back((8, 1), 8) + back((4, 1), 4, via_b)
            totals.append(jnp.stack([g_a, g_b]))
        d_down = jnp.concatenate([totals[2][:, h * ff:(h + 1) * ff] for h in range(dim // ff)], axis=2)
        return y_tok, dx_tok, totals[0], totals[1], d_down

    return jax.shard_map(layer, mesh=mesh, in_specs=(P('ep'),) * 7, out_specs=(P('ep'),) * 5, check_vma=False)
```

```python
import functools

import jax
import jax.numpy as jnp
from jax import lax
from jax.experimental import pallas as pl
from jax.experimental.pallas import tpu as pltpu
from jax.sharding import PartitionSpec as P


BF = jnp.bfloat16
F32 = jnp.float32
I32 = jnp.int32
TILE = 256
GROUP = 16
DEPTH = 4
KEY_STEP = 4096
LIST_PART = 1024
GRANT = 62 * 1024 * 1024
EXPERTS = ((4, 0), (8, 1), (0, 0), (0, 1), (8, 0), (4, 1), (12, 0), (12, 1))
CALLS = ((0, 0, 4), (1, 0, 2), (1, 2, 6), (1, 6, 8), (0, 6, 8), (0, 4, 6))
DEFERRED = 2
HBM = pl.BlockSpec(memory_space=pltpu.HBM)
DMA = pltpu.SemaphoreType.DMA


def dot_nt(lhs, rhs):
    return lax.dot_general(lhs, rhs, (((1,), (1,)), ((), ())), preferred_element_type=F32)


def dot_tn(lhs, rhs):
    return lax.dot_general(lhs, rhs, (((0,), (0,)), ((), ())), preferred_element_type=F32)


def dot_nn(lhs, rhs):
    return jnp.dot(lhs, rhs, preferred_element_type=F32)


def start_all(copies):
    for copy in copies:
        copy.start()


def wait_all(copies):
    for copy in copies:
        copy.wait()


def tile_rows(t):
    return pl.ds(pl.multiple_of(t * TILE, TILE), TILE)


def pack_kernel(ff, gate_ref, up_ref, down_ref, a_out, b_out, w_buf, w_in, w_out):
    dim = gate_ref.shape[1]
    loads, stores = [], []
    for e, out in enumerate((a_out, b_out)):
        parts = [(gate_ref.at[e], 0, dim), (up_ref.at[e], dim, dim)]
        parts += [(down_ref.at[e, :, pl.ds(h * ff, ff)], 2 * dim + h * ff, ff) for h in range(dim // ff)]
        for i, (src, row, size) in enumerate(parts):
            place = pl.ds(row, size)
            loads.append(pltpu.make_async_copy(src, w_buf.at[e, place], w_in.at[e, i]))
            stores.append(pltpu.make_async_copy(w_buf.at[e, place], out.at[place], w_out.at[e, i]))
    start_all(loads)
    for load, store in zip(loads, stores):
        load.wait()
        store.start()
    wait_all(stores)


def prep_kernel(x_ref, dy_ref, xd0_out, xd1_out, rows, xd, stage, in_sems, out_sems):
    tok_loc, dim = x_ref.shape
    lanes = dim // 128
    blocks = tok_loc // TILE
    loads = [[pltpu.make_async_copy(ref.at[tile_rows(b)], rows.at[i, tile_rows(b)], in_sems.at[i, b]) for i, ref in enumerate((x_ref, dy_ref))] for b in range(blocks)]
    for pair in loads:
        start_all(pair)
    stores = []
    for b in range(blocks):
        wait_all(loads[b])
        for i in range(2):
            for c in range(lanes):
                stage[i, pl.ds(c, TILE, stride=lanes), :] = rows[i, tile_rows(b), c * 128:(c + 1) * 128].astype(F32)
            xd[tile_rows(b), i * lanes:(i + 1) * lanes, :] = stage[i].reshape(TILE, lanes, 128).astype(BF)
        out, first = (xd0_out, 0) if b < blocks // 2 else (xd1_out, blocks // 2)
        stores.append(pltpu.make_async_copy(xd.at[tile_rows(b)], out.at[tile_rows(b - first)], out_sems.at[b]))
        stores[-1].start()
    wait_all(stores)


def list_stream(first, count, tok_hbm, gate_hbm, tok, gate, sems):
    per_part = LIST_PART // TILE

    def copies(c):
        part = pl.ds(pl.multiple_of(c * LIST_PART, LIST_PART), LIST_PART)
        return (pltpu.make_async_copy(tok_hbm.at[part], tok.at[part], sems.at[0, c]),
                pltpu.make_async_copy(gate_hbm.at[part], gate.at[part], sems.at[1, c]))

    def start(c, carry):
        start_all(copies(c))
        return carry

    def wait(t):
        @pl.when((t == first) | (lax.rem(t, per_part) == 0))
        def _():
            wait_all(copies(lax.div(t, per_part)))

    lax.fori_loop(lax.div(first, per_part), lax.div(first + count + per_part - 1, per_part), start, 0)
    return wait


def table_copies(pieces, table, sems):
    size, _ = pieces[0].shape
    return [pltpu.make_async_copy(ref, table.at[pl.ds(i * size, size)], sems.at[i]) for i, ref in enumerate(pieces)]


def gather_tile(lanes, t, table, tok, gate, x_stage, g_stage, x_dst, g_dst):
    half = lanes // 2

    def body(block, carry):
        row0 = block * GROUP
        for q in range(0, GROUP, 2):
            pos = t * TILE + row0 + q
            pair = [table[pl.ds(pl.multiple_of(tok[pos + i], 2 * lanes), 2 * lanes), :] for i in range(2)]
            x_pair = [both[:lanes].astype(F32) for both in pair]
            g_pair = [both[lanes:].astype(F32) * gate[pos + i] for i, both in enumerate(pair)]
            for stage, rows in ((x_stage, x_pair), (g_stage, g_pair)):
                for h in range(2):
                    dst = pl.ds(pl.multiple_of((row0 + q) * half, lanes), lanes)
                    stage[h, dst, :] = jnp.concatenate([row[h * half:(h + 1) * half] for row in rows], axis=0)
        return carry

    lax.fori_loop(0, TILE // GROUP, body, 0)
    for c in range(lanes):
        cols = slice(c * 128, (c + 1) * 128)
        src = (c // half, pl.ds(c % half, TILE, stride=half))
        x_dst[:, cols] = x_stage[src].astype(BF)
        g_dst[:, cols] = g_stage[src].astype(BF)


def gather_kernel(lanes, total, tok_hbm, gate_hbm, *rest):
    pieces = rest[:4]
    x_out, g_out, table, x_stage, g_stage, x_buf, g_buf, tok, gate, sems, out_sems, list_sems = rest[4:]
    count = total[0]
    list_wait = list_stream(0, count, tok_hbm, gate_hbm, tok, gate, list_sems)
    copies = table_copies(pieces, table, sems)
    start_all(copies)
    pad_rows = pl.ds(table.shape[0] - 16 * lanes, 2 * lanes)
    table[pad_rows, :] = jnp.zeros((2 * lanes, 128), BF)
    wait_all(copies)

    def stores(t, slot):
        return (pltpu.make_async_copy(x_buf.at[slot], x_out.at[tile_rows(t)], out_sems.at[0, slot]),
                pltpu.make_async_copy(g_buf.at[slot], g_out.at[tile_rows(t)], out_sems.at[1, slot]))

    def tile(t, carry):
        slot = lax.rem(t, DEPTH)
        list_wait(t)

        @pl.when(t >= DEPTH)
        def _():
            wait_all(stores(t - DEPTH, slot))

        gather_tile(lanes, t, table, tok, gate, x_stage, g_stage, x_buf.at[slot], g_buf.at[slot])
        start_all(stores(t, slot))
        return carry

    lax.fori_loop(0, count, tile, 0)
    for back in range(DEPTH, 0, -1):
        @pl.when(count >= back)
        def _():
            wait_all(stores(count - back, lax.rem(count - back, DEPTH)))


def grad_parts(key):
    return 1 if key in EXPERTS[:2] else 3


def part_refs(refs, dim):
    return [refs[0].at[pl.ds(c * dim, dim)] for c in range(3)] if len(refs) == 1 else refs


def row_math(ff, dim, x_rows, g_rows, w_ref, o_dst, dx_dst):
    gate_w = w_ref[0:dim, :]
    up_w = w_ref[dim:2 * dim, :]
    u_val = dot_nn(x_rows, gate_w)
    v_val = dot_nn(x_rows, up_w)
    sig = jax.nn.sigmoid(u_val)
    act = (u_val * sig * v_val).astype(BF)
    d_act = None
    for h in range(dim // ff):
        cols = slice(h * ff, (h + 1) * ff)
        down = w_ref[2 * dim + h * ff:2 * dim + (h + 1) * ff, :]
        o_dst[:, cols] = dot_nn(act, down).astype(BF)
        part = dot_nt(g_rows[:, cols], down)
        d_act = part if d_act is None else d_act + part
    d_u = (d_act * v_val * sig * (1.0 + u_val * (1.0 - sig))).astype(BF)
    d_v = (d_act * u_val * sig).astype(BF)
    dx_dst[...] = (dot_nt(d_u, gate_w) + dot_nt(d_v, up_w)).astype(BF)
    return act, d_u, d_v


def add_grads(ff, dim, p_ref, x_rows, g_rows, act, d_u, d_v):
    p_ref[0:dim, :] += dot_tn(x_rows, d_u)
    p_ref[dim:2 * dim, :] += dot_tn(x_rows, d_v)
    for h in range(dim // ff):
        p_ref[2 * dim + h * ff:2 * dim + (h + 1) * ff, :] += dot_tn(act, g_rows[:, h * ff:(h + 1) * ff])


def deferring_kernel(ff, dim, j0, n, first_tile, n_tiles, x_hbm, g_hbm, *rest):
    w_refs = rest[:n]
    o_hbm, dx_hbm, f_hbm, w_buf, x_buf, g_buf, o_buf, dx_buf, f_buf, w_sem, in_sem, out_sem = rest[n + 2:]
    base = first_tile[j0]
    count = first_tile[j0 + n - 1] + n_tiles[j0 + n - 1] - base

    def loads(t, slot):
        rows = tile_rows(base + t)
        return [pltpu.make_async_copy(ref.at[rows], buf.at[slot], in_sem.at[i, slot]) for i, (ref, buf) in enumerate(((x_hbm, x_buf), (g_hbm, g_buf)))]

    def stores(t, slot):
        rows = tile_rows(base + t)
        return [pltpu.make_async_copy(buf.at[slot], ref.at[rows], out_sem.at[i, slot]) for i, (ref, buf) in enumerate(((o_hbm, o_buf), (dx_hbm, dx_buf), (f_hbm, f_buf)))]

    def w_copy(i):
        return pltpu.make_async_copy(w_refs[i], w_buf.at[i % 2], w_sem.at[i % 2])

    start_all(loads(0, 0))
    w_copy(0).start()

    def tile(t, carry):
        slot = lax.rem(t, 2)
        place = base + t
        which = jnp.int32(0)
        for i in range(1, n):
            which = which + (place >= first_tile[j0 + i]).astype(I32)

        @pl.when(t + 1 < count)
        def _():
            start_all(loads(t + 1, 1 - slot))

        for i in range(n):
            @pl.when(place == first_tile[j0 + i])
            def _():
                w_copy(i).wait()
                if i < n - 1:
                    w_copy(i + 1).start()

        @pl.when(t >= 2)
        def _():
            wait_all(stores(t - 2, slot))

        wait_all(loads(t, slot))
        factors = row_math(ff, dim, x_buf[slot], g_buf[slot], w_buf.at[lax.rem(which, 2)], o_buf.at[slot], dx_buf.at[slot])
        for c, value in enumerate(factors):
            f_buf[slot, :, c * ff:(c + 1) * ff] = value
        start_all(stores(t, slot))
        return carry

    lax.fori_loop(0, count, tile, 0)
    for back in (2, 1):
        @pl.when(count >= back)
        def _():
            wait_all(stores(count - back, lax.rem(count - back, 2)))


def late_grad_kernel(ff, dim, j0, n, first_tile, n_tiles, x_hbm, g_hbm, f_hbm, *rest):
    init_refs = [rest[3 * i:3 * i + 3] for i in range(n)]
    p_refs = [rest[3 * (n + i):3 * (n + i) + 3] for i in range(n)]
    p_buf, x_buf, g_buf, f_buf, i_sem, p_sem, in_sem = rest[6 * n:]
    base = first_tile[j0]
    count = first_tile[j0 + n - 1] + n_tiles[j0 + n - 1] - base

    def loads(t, slot):
        rows = tile_rows(base + t)
        return [pltpu.make_async_copy(ref.at[rows], buf.at[slot], in_sem.at[i, slot]) for i, (ref, buf) in enumerate(((x_hbm, x_buf), (g_hbm, g_buf), (f_hbm, f_buf)))]

    def moves(refs, i, sem, out):
        pairs = [(refs[i][c], p_buf.at[i % 3, pl.ds(c * dim, dim)], sem.at[i % 3, c]) for c in range(3)]
        return [pltpu.make_async_copy(vmem, hbm, s) if out else pltpu.make_async_copy(hbm, vmem, s) for hbm, vmem, s in pairs]

    start_all(loads(0, 0))
    start_all(moves(init_refs, 0, i_sem, False))

    def tile(t, carry):
        slot = lax.rem(t, 2)
        place = base + t
        which = jnp.int32(0)
        for i in range(1, n):
            which = which + (place >= first_tile[j0 + i]).astype(I32)

        @pl.when(t + 1 < count)
        def _():
            start_all(loads(t + 1, 1 - slot))

        for i in range(n):
            @pl.when(place == first_tile[j0 + i])
            def _():
                if i >= 2:
                    wait_all(moves(p_refs, i - 2, p_sem, True))
                if i < n - 1:
                    start_all(moves(init_refs, i + 1, i_sem, False))
                wait_all(moves(init_refs, i, i_sem, False))

        wait_all(loads(t, slot))
        factors = [f_buf[slot, :, c * ff:(c + 1) * ff] for c in range(3)]
        add_grads(ff, dim, p_buf.at[lax.rem(which, 3)], x_buf[slot], g_buf[slot], *factors)

        for i in range(n):
            @pl.when(place == first_tile[j0 + i] + n_tiles[j0 + i] - 1)
            def _():
                start_all(moves(p_refs, i, p_sem, True))
        return carry

    lax.fori_loop(0, count, tile, 0)
    for i in range(max(0, n - 2), n):
        wait_all(moves(p_refs, i, p_sem, True))


def expert_kernel(ff, dim, j0, n, inits, n_carried, first_tile, n_tiles, *rest):
    ins, rest = rest[:2], rest[2:]
    w_refs = rest[:n]
    rest = list(rest[n:])

    def take(key):
        return part_refs([rest.pop(0) for _ in range(grad_parts(key))], dim)

    keys = EXPERTS[j0:j0 + n]
    init_refs = [take(key) if has else None for key, has in zip(keys, inits)]
    rest = rest[n_carried:]
    o_hbm, dx_hbm, *rest = rest
    p_refs = [take(key) for key in keys]
    w_buf, p_buf, x_buf, g_buf, o_buf, dx_buf, w_sem, i_sem, p_sem, in_sem, out_sem = rest
    base = first_tile[j0]
    count = first_tile[j0 + n - 1] + n_tiles[j0 + n - 1] - base

    def loads(t, slot):
        rows = tile_rows(base + t)
        return [pltpu.make_async_copy(ref.at[rows], buf.at[slot], in_sem.at[i, slot]) for i, (ref, buf) in enumerate(zip(ins, (x_buf, g_buf)))]

    def stores(t, slot):
        rows = tile_rows(base + t)
        return (pltpu.make_async_copy(o_buf.at[slot], o_hbm.at[rows], out_sem.at[0, slot]),
                pltpu.make_async_copy(dx_buf.at[slot], dx_hbm.at[rows], out_sem.at[1, slot]))

    def w_copy(i):
        return pltpu.make_async_copy(w_refs[i], w_buf.at[i % 2], w_sem.at[i % 2])

    def init_copy(i):
        return [pltpu.make_async_copy(init_refs[i][c], p_buf.at[i % 3, pl.ds(c * dim, dim)], i_sem.at[i % 3, c]) for c in range(3)]

    def flush(i):
        return [pltpu.make_async_copy(p_buf.at[i % 3, pl.ds(c * dim, dim)], p_refs[i][c], p_sem.at[i % 3, c]) for c in range(3)]

    start_all(loads(0, 0))
    w_copy(0).start()

    def tile(t, carry):
        slot = lax.rem(t, 2)
        place = base + t
        which = jnp.int32(0)
        for i in range(1, n):
            which = which + (place >= first_tile[j0 + i]).astype(I32)

        @pl.when(t + 1 < count)
        def _():
            start_all(loads(t + 1, 1 - slot))

        for i in range(n):
            @pl.when(place == first_tile[j0 + i])
            def _():
                w_copy(i).wait()
                if i == 0 and inits[0]:
                    start_all(init_copy(0))
                if i < n - 1:
                    w_copy(i + 1).start()
                if i >= 2:
                    wait_all(flush(i - 2))
                if i < n - 1 and inits[i + 1]:
                    start_all(init_copy(i + 1))
                if not inits[i]:
                    def clear(r, inner):
                        p_buf[i % 3, pl.ds(pl.multiple_of(r * 64, 64), 64), :] = jnp.zeros((64, ff), F32)
                        return inner

                    lax.fori_loop(0, 3 * dim // 64, clear, 0)

        @pl.when(t >= 2)
        def _():
            wait_all(stores(t - 2, slot))

        wait_all(loads(t, slot))
        factors = row_math(ff, dim, x_buf[slot], g_buf[slot], w_buf.at[lax.rem(which, 2)], o_buf.at[slot], dx_buf.at[slot])
        start_all(stores(t, slot))
        for i in range(n):
            if inits[i]:
                @pl.when(place == first_tile[j0 + i])
                def _():
                    wait_all(init_copy(i))
        add_grads(ff, dim, p_buf.at[lax.rem(which, 3)], x_buf[slot], g_buf[slot], *factors)

        for i in range(n):
            @pl.when(place == first_tile[j0 + i] + n_tiles[j0 + i] - 1)
            def _():
                start_all(flush(i))
        return carry

    lax.fori_loop(0, count, tile, 0)
    for back in (2, 1):
        @pl.when(count >= back)
        def _():
            wait_all(stores(count - back, lax.rem(count - back, 2)))
    for i in range(max(0, n - 2), n):
        wait_all(flush(i))


def combine_kernel(lanes, n_src, use_gate, total, tok_hbm, gate_hbm, rows_hbm, mate_out, own_out, acc, stage, buf, tok, gate, sems, in_sem, list_sems):
    count = total[0]
    list_wait = list_stream(0, count, tok_hbm, gate_hbm, tok, gate, list_sems)

    def load(t, slot):
        return pltpu.make_async_copy(rows_hbm.at[tile_rows(t)], buf.at[slot], in_sem.at[slot])

    for ahead in range(DEPTH - 1):
        @pl.when(ahead < count)
        def _():
            load(ahead, ahead).start()

    def clear(i, carry):
        acc[pl.ds(pl.multiple_of(i * 256, 256), 256), :] = jnp.zeros((256, 128), F32)
        return carry

    lax.fori_loop(0, acc.shape[0] // 256, clear, 0)

    def tile(t, carry):
        slot = lax.rem(t, DEPTH)

        @pl.when(t + DEPTH - 1 < count)
        def _():
            load(t + DEPTH - 1, lax.rem(t + DEPTH - 1, DEPTH)).start()

        list_wait(t)
        load(t, slot).wait()
        for c in range(lanes):
            stage[pl.ds(c, TILE, stride=lanes), :] = buf[slot, :, c * 128:(c + 1) * 128].astype(F32)

        def body(block, inner):
            row0 = block * GROUP
            dests, sums = [], []
            for q in range(GROUP):
                pos = t * TILE + row0 + q
                t_row = pl.ds(pl.multiple_of(tok[pos], lanes), lanes)
                value = stage[pl.ds(pl.multiple_of((row0 + q) * lanes, lanes), lanes), :]
                if use_gate:
                    value = value * gate[pos]
                dests.append(t_row)
                sums.append(acc[t_row, :] + value)
            for t_row, total_row in zip(dests, sums):
                acc[t_row, :] = total_row
            return inner

        lax.fori_loop(0, TILE // GROUP, body, 0)
        return carry

    lax.fori_loop(0, count, tile, 0)
    copies = [pltpu.make_async_copy(acc.at[pl.ds(i * n_src * lanes, n_src * lanes)], ref, sems.at[i]) for i, ref in enumerate((mate_out, own_out))]
    start_all(copies)
    wait_all(copies)


def add_kernel(a_ref, b_ref, out_ref):
    out_ref[...] = a_ref[...] + b_ref[...]


def finish_kernel(lanes, near_ref, x_ref, out_ref, stage):
    rows = near_ref.shape[0] // lanes
    stage[...] = near_ref[...] + x_ref[...]
    for c in range(lanes):
        out_ref[:, c * 128:(c + 1) * 128] = stage[pl.ds(c, rows, stride=lanes), :].astype(BF)


def total_kernel(near_a, far_a, near_b, far_b, out_ref):
    for e, (near, far) in enumerate(((near_a, far_a), (near_b, far_b))):
        value = near[...] + far[...]
        out_ref[e] = jnp.concatenate([value[h] for h in range(value.shape[0])], axis=1)


def solution(mesh):
    n_dev = mesh.shape['ep']

    def permute(value, mask):
        return lax.ppermute(value, 'ep', [(i, i ^ mask) for i in range(n_dev)])

    def call_kernel(body, args, scalars, out_shape, scratch, aliases=None):
        spec = pltpu.PrefetchScalarGridSpec(num_scalar_prefetch=len(scalars), grid=(), in_specs=[HBM] * len(args), out_specs=[HBM] * len(out_shape), scratch_shapes=scratch)
        return pl.pallas_call(body, grid_spec=spec, out_shape=out_shape, input_output_aliases=aliases or {},
                              compiler_params=pltpu.CompilerParams(vmem_limit_bytes=GRANT))(*scalars, *args)

    def layer(x_tok, route_idx, gates, dy_tok, w_gate, w_up, w_down):
        tok_loc, top_k = route_idx.shape
        dim, ff = w_gate.shape[1], w_gate.shape[2]
        experts = w_gate.shape[0] * n_dev
        lanes = dim // 128
        n_exp = len(EXPERTS)
        slot_cap = max(2 * tok_loc * top_k // (experts - 2), tok_loc // 2)
        list_len = n_exp * -(-2 * slot_cap // TILE) * TILE
        n_half = 2 * tok_loc
        me = lax.axis_index('ep')

        w_shape = jax.ShapeDtypeStruct((3 * dim, ff), BF)
        xd_shape = jax.ShapeDtypeStruct((tok_loc // 2, 2 * lanes, 128), BF)
        own_a, own_b = call_kernel(
            functools.partial(pack_kernel, ff), (w_gate, w_up, w_down), (), [w_shape, w_shape], [pltpu.VMEM((2, 3 * dim, ff), BF), DMA((2, 4)), DMA((2, 4))])
        xd_own = call_kernel(
            prep_kernel, (x_tok, dy_tok), (), [xd_shape, xd_shape],
            [pltpu.VMEM((2, tok_loc, dim), BF), pltpu.VMEM((tok_loc, 2 * lanes, 128), BF), pltpu.VMEM((2, TILE * lanes, 128), F32), DMA((2, tok_loc // TILE)), DMA((tok_loc // TILE,))])
        routing = jnp.concatenate([route_idx.T.astype(F32), gates.T.astype(F32)], axis=0)
        rt_xp = permute(routing, 2)
        rt_mate = permute(routing, 1)
        rt_xpm = permute(rt_xp, 1)
        xd_own = [part.reshape(-1, 128) for part in xd_own]
        wts = {(0, 0): own_a, (0, 1): own_b}
        for key, via, mask in (((4, 0), (0, 0), 4), ((8, 1), (0, 1), 8), ((4, 1), (0, 1), 4), ((8, 0), (0, 0), 8), ((12, 0), (8, 0), 4), ((12, 1), (4, 1), 8)):
            wts[key] = permute(wts[via], mask)
        xd_xp = [permute(part, 2) for part in xd_own]
        xd_mate = [permute(part, 1) for part in xd_own]
        xd_xpm = [permute(part, 1) for part in xd_xp]

        rt_all = jnp.stack([jnp.stack([rt_mate, routing]), jnp.stack([rt_xpm, rt_xp])])
        route = rt_all[:, :, :top_k].astype(I32)
        gate_in = rt_all[:, :, top_k:]
        place = (route // 2) ^ me
        slot = jnp.full_like(route, n_exp)
        for j, (mask, which) in enumerate(EXPERTS):
            slot = jnp.where((place == mask) & (route % 2 == which), j, slot)
        token = lax.broadcasted_iota(I32, route.shape, 1) * tok_loc + lax.broadcasted_iota(I32, route.shape, 3)
        first_key = jnp.arange(2, dtype=I32) * (16 * KEY_STEP)
        key = (slot * KEY_STEP + token + first_key[:, None, None, None]).reshape(2, -1)
        counts = jnp.sum((slot.reshape(1, 2, -1) == jnp.arange(n_exp).reshape(n_exp, 1, 1)).astype(I32), axis=2).T
        n_tiles = jnp.maximum(1, (counts + TILE - 1) // TILE)
        need = n_tiles * TILE - counts
        pad_key = jnp.where(jnp.arange(TILE) < need[:, :, None], jnp.arange(n_exp)[:, None] * KEY_STEP + n_half, n_exp * KEY_STEP) + first_key[:, None, None]
        keys = jnp.concatenate([key, pad_key.reshape(2, -1)], axis=1)
        vals = jnp.concatenate([gate_in.reshape(2, -1), jnp.zeros((2, n_exp * TILE), F32)], axis=1)
        keys, vals = lax.sort((keys.reshape(-1), vals.reshape(-1)), num_keys=1)
        per_half = n_half * top_k + n_exp * TILE
        tile_ends = jnp.cumsum(n_tiles, axis=1)
        totals = [tile_ends[h, n_exp - 1:] for h in range(2)]
        toks = [keys[h * per_half:][:list_len] & (KEY_STEP - 1) for h in range(2)]
        lists = [(toks[h] * (2 * lanes), vals[h * per_half:][:list_len]) for h in range(2)]
        places = [tok * lanes for tok in toks]
        tiles = [(tile_ends[h] - n_tiles[h], n_tiles[h]) for h in range(2)]

        row_shape = jax.ShapeDtypeStruct((list_len, dim), BF)
        tile_buf = pltpu.VMEM((2, TILE, dim), BF)
        factor_shape = jax.ShapeDtypeStruct((list_len, 3 * ff), BF)
        factor_buf = pltpu.VMEM((2, TILE, 3 * ff), BF)
        deep_buf = pltpu.VMEM((DEPTH, TILE, dim), BF)
        half_buf = pltpu.VMEM((2, TILE * lanes // 2, 128), F32)
        list_bufs = [pltpu.SMEM((list_len,), I32), pltpu.SMEM((list_len,), F32)]
        list_sems = DMA((2, list_len // LIST_PART))
        table = pltpu.VMEM(((n_half + 8) * 2 * lanes, 128), BF)
        ins = [call_kernel(
            functools.partial(gather_kernel, lanes), (*lists[h], *pieces), (totals[h],), [row_shape, row_shape],
            [table, half_buf, half_buf, deep_buf, deep_buf, *list_bufs, DMA((4,)), DMA((2, DEPTH)), list_sems])
            for h, pieces in enumerate(((*xd_mate, *xd_own), (*xd_xpm, *xd_xp)))]

        grads, outs = {}, [(), ()]
        for i, (half, lo, hi) in enumerate(CALLS):
            n, keys_now = hi - lo, EXPERTS[lo:hi]
            given = [part for k in keys_now if k in grads for part in grads[k]]
            args = [*ins[half], *[wts[k] for k in keys_now], *given, *outs[half]]
            first_alias = 2 + len(args) - 2
            grad_shapes = [jax.ShapeDtypeStruct((3 * dim // grad_parts(k), ff), F32) for k in keys_now for _ in range(grad_parts(k))]
            scratch = [pltpu.VMEM((2, 3 * dim, ff), BF), pltpu.VMEM((3, 3 * dim, ff), F32), tile_buf, tile_buf, tile_buf, tile_buf,
                       DMA((2,)), DMA((3, 3)), DMA((3, 3)), DMA((2, 2)), DMA((2, 2))]
            aliases = {first_alias: 0, first_alias + 1: 1} if outs[half] else None
            if i == DEFERRED:
                args = [*ins[half], *[wts[k] for k in keys_now], *outs[half]]
                *outs[half], factors = call_kernel(
                    functools.partial(deferring_kernel, ff, dim, lo, n), args, tiles[half], [row_shape, row_shape, factor_shape],
                    [pltpu.VMEM((2, 3 * dim, ff), BF), tile_buf, tile_buf, tile_buf, tile_buf, factor_buf, DMA((2,)), DMA((2, 2)), DMA((3, 2))],
                    {2 + n + 2: 0, 2 + n + 3: 1})
                continue
            body = functools.partial(expert_kernel, ff, dim, lo, n, tuple(k in grads for k in keys_now), len(outs[half]))
            parts = call_kernel(body, args, tiles[half], [row_shape, row_shape] + grad_shapes, scratch, aliases)
            outs[half], parts = parts[:2], parts[2:]
            for k in keys_now:
                grads[k], parts = tuple(parts[:grad_parts(k)]), parts[grad_parts(k):]
        half, lo, hi = CALLS[DEFERRED]
        late = EXPERTS[lo:hi]
        parts = call_kernel(
            functools.partial(late_grad_kernel, ff, dim, lo, hi - lo), [*ins[half], factors, *[part for k in late for part in grads[k]]], tiles[half],
            [jax.ShapeDtypeStruct((dim, ff), F32)] * (3 * (hi - lo)),
            [pltpu.VMEM((3, 3 * dim, ff), F32), tile_buf, tile_buf, factor_buf, DMA((3, 3)), DMA((3, 3)), DMA((3, 2))])
        for m, k in enumerate(late):
            grads[k] = tuple(parts[3 * m:3 * m + 3])

        def combine(half, which, use_gate):
            block = jax.ShapeDtypeStruct((tok_loc * lanes, 128), F32)
            return call_kernel(
                functools.partial(combine_kernel, lanes, tok_loc, use_gate), (places[half], lists[half][1], outs[half][which]), (totals[half],), [block, block],
                [pltpu.VMEM(((n_half + 32) * lanes, 128), F32), pltpu.VMEM((TILE * lanes, 128), F32), deep_buf, *list_bufs, DMA((2,)), DMA((DEPTH,)), list_sems])

        def blocked(body, args, out_shape, in_block, out_block, steps, scratch=()):
            def spec(block):
                axis = 1 if len(block) == 3 else 0
                return pl.BlockSpec(block, lambda i: tuple(i if d == axis else 0 for d in range(len(block))))

            return pl.pallas_call(body, grid=(steps,), in_specs=[spec(in_block)] * len(args), out_specs=spec(out_block), out_shape=out_shape, scratch_shapes=scratch,
                                  compiler_params=pltpu.CompilerParams(vmem_limit_bytes=GRANT))(*args)

        row_block = (TILE * lanes, 128)
        steps = tok_loc // TILE

        def settle_rows(which, use_gate):
            mate1, own1 = combine(1, which, use_gate)
            to_x = blocked(add_kernel, (own1, permute(mate1, 1)), jax.ShapeDtypeStruct((tok_loc * lanes, 128), F32), row_block, row_block, steps)
            from_x = permute(to_x, 2)
            mate0, own0 = combine(0, which, use_gate)
            near_sum = own0 + permute(mate0, 1)
            return blocked(functools.partial(finish_kernel, lanes), (near_sum, from_x), jax.ShapeDtypeStruct((tok_loc, dim), BF), row_block, (TILE, dim), steps,
                           (pltpu.VMEM((TILE * lanes, 128), F32),))

        y_tok = settle_rows(0, True)
        dx_tok = settle_rows(1, False)

        whole_a = permute(grads[(4, 0)][0], 4)
        whole_b = permute(grads[(8, 1)][0], 8)
        sums = []
        for c in range(3):
            def back(key, mask, value=None):
                return permute(grads[key][c] if value is None else value, mask)

            via_a = grads[(8, 0)][c] + back((12, 0), 4)
            via_b = grads[(4, 1)][c] + back((12, 1), 8)
            part = slice(c * dim, (c + 1) * dim)
            near_a = grads[(0, 0)][c] + whole_a[part]
            near_b = grads[(0, 1)][c] + whole_b[part]
            parts = (near_a, back((8, 0), 8, via_a), near_b, back((4, 1), 4, via_b))
            wide = dim // ff if c == 2 else 1
            rows = dim // wide
            sums.append(blocked(total_kernel, [p.reshape(wide, rows, ff) for p in parts], jax.ShapeDtypeStruct((2, rows, wide * ff), F32),
                                (wide, 128, ff), (2, 128, wide * ff), rows // 128))
        return y_tok, dx_tok, *sums

    return jax.shard_map(layer, mesh=mesh, in_specs=(P('ep'),) * 7, out_specs=(P('ep'),) * 5, check_vma=False)
```
